32 devices in a mesh: groups: 2 (over y), seq: 4 (over z), head: 4 (over x, core).
Axes of the slice: x: 2, y: 2, z: 4, core: 2. Of those that a mesh axis runs over, the one named last changes fastest.
Arguments:
- queries: bfloat16 [32, 3, 32, 128], P('groups', None, 'head'), parts along dimension 0, may hold values from -8 to 8
- new_kv: bfloat16 [4, 16, 3, 4, 128], P('groups', None, None, 'head'), parts along dimension 0, may hold values from -16 to 16
- res_kv: bfloat16 [4, 2, 16384, 4, 128], P('groups', None, 'seq', 'head'), parts along dimension 0, may hold values from -16 to 16
- prefill_kv: bfloat16 [4, 4, 4096, 128], P('groups', None, ('seq', 'head')), parts along dimension 0, may hold values from -16 to 16
- block_table: int32 [128], P('groups'), parts along dimension 0, may hold values from 0 to 63, as said below
- lengths: int32 [6], P('groups'), parts along dimension 0, may hold values from 4096 to 16384, as said below
- join_step: int32 [2], P('groups'), parts along dimension 0, may hold values from 1 to 15
Outputs:
- attn_out: bfloat16 [32, 3, 32, 128], P('groups', None, 'head'), parts along dimension 0
- new_cache: bfloat16 [4, 4, 4096, 128], P('groups', 'head', 'seq'), parts along dimension 0
The draws below stay inside these ranges and needn't reach their ends.
There are 2 independent parts, one for each index of `groups`. The reference program is written for one: setup_inputs(seed, part) draws one part's arguments, and reference() takes and returns one part's arrays. A program takes and returns all parts, laid end to end along the dimension named above; each array names one. Nothing has to cross between parts.
Inputs may be any that keep to these rules, and one draw needn't show every extreme that they name: `block_table`: A permutation of 0 to 63. In each aligned run of 4 entries (the blocks of one prefill device) every aligned range of 16 slots is named exactly 1 times. `lengths`: entries 0 to 1 lie between 4096 and 16384, and one of them equals 16384; entry 2 equals 4096.
All inputs are finite; a program needn't handle non-finite values.
Results may differ from the reference program's by a relative error of at most 0.0039.
Values may be sent and summed in bfloat16 or wider, within the bound.
A program may use at most 64 MiB of HBM per device.

```python
import math
import jax
import jax.numpy as jnp
from jax import lax

HD = 128
QPK = 8
RES = 2
STEPS = 16
BLOCK = 64
PAGES = 1
KVH = 4
QH = 32
DEV_BLOCKS = 4
LNEW = 4096
NBLK = 64
RES_LEN = 16384


def query_values(key):
    array_shape = (STEPS, RES + 1, QH, HD)
    base_draw = jax.random.normal(jax.random.fold_in(key, 31), array_shape, jnp.float32)
    return jnp.clip(base_draw, -8.0, 8.0)


def draw_queries(key, part):
    return query_values(key).astype(jnp.bfloat16)


def draw_new_kv(key, part):
    array_shape = (STEPS, RES + 1, KVH, HD)
    centre = query_values(key).reshape(STEPS, RES + 1, KVH, QPK, HD).mean(axis=3)
    key_part = 9.0 * centre + 1.5 * jax.random.normal(jax.random.fold_in(key, 51), array_shape, jnp.float32)
    value_part = jax.random.normal(jax.random.fold_in(key, 52), array_shape, jnp.float32)
    return jnp.clip(jnp.stack([key_part, value_part]), -16.0, 16.0).astype(jnp.bfloat16)


def draw_res_kv(key, part):
    array_shape = (RES, RES_LEN, KVH, HD)
    key_part = 3.0 * jax.random.normal(jax.random.fold_in(key, 11), array_shape, jnp.float32)
    value_part = jax.random.normal(jax.random.fold_in(key, 12), array_shape, jnp.float32)
    return jnp.clip(jnp.stack([key_part, value_part]), -16.0, 16.0).astype(jnp.bfloat16)


def draw_prefill_kv(key, part):
    array_shape = (KVH, LNEW, HD)
    key_part = 3.0 * jax.random.normal(jax.random.fold_in(key, 13), array_shape, jnp.float32)
    value_part = jax.random.normal(jax.random.fold_in(key, 14), array_shape, jnp.float32)
    return jnp.clip(jnp.stack([key_part, value_part]), -16.0, 16.0).astype(jnp.bfloat16)


def shuffle_pattern(sub_key, pattern):
    return jax.random.permutation(sub_key, pattern)


def draw_block_table(key, part):
    shard_count = DEV_BLOCKS // PAGES
    sender_count = NBLK // DEV_BLOCKS
    pattern = jnp.repeat(jnp.arange(shard_count, dtype=jnp.int32), PAGES)
    sender_keys = jax.random.split(jax.random.fold_in(key, 41), sender_count)
    shard_of = jax.vmap(shuffle_pattern, in_axes=(0, None))(sender_keys, pattern).reshape(-1).astype(jnp.int32)
    priority = jax.random.permutation(jax.random.fold_in(key, 42), NBLK).astype(jnp.int32)
    ordering = jnp.argsort(shard_of * NBLK + priority, stable=True).astype(jnp.int32)
    return jnp.zeros((NBLK,), jnp.int32).at[ordering].set(jnp.arange(NBLK, dtype=jnp.int32))


def draw_lengths(key, part):
    resident = jax.random.randint(jax.random.fold_in(key, 61), (RES,), RES_LEN // 4, RES_LEN + 1)
    full_one = jax.random.randint(jax.random.fold_in(key, 63), (), 0, RES)
    resident = jnp.where(jnp.arange(RES, dtype=jnp.int32) == full_one, RES_LEN, resident)
    joining = jnp.full((1,), LNEW, jnp.int32)
    return jnp.concatenate([resident.astype(jnp.int32), joining]).astype(jnp.int32)


def setup_inputs(seed: int = 0, part: int = 0) -> dict:
    key_of = jax.random.split(jax.random.key(seed), 8)
    part_keys = jax.random.split(jax.random.fold_in(key_of[7], part), 8)
    return {
        "queries": draw_queries(jax.random.fold_in(jax.random.fold_in(key_of[7], part), 71), part),
        "new_kv": draw_new_kv(jax.random.fold_in(jax.random.fold_in(key_of[7], part), 71), part),
        "res_kv": draw_res_kv(jax.random.fold_in(jax.random.fold_in(key_of[7], part), 71), part),
        "prefill_kv": draw_prefill_kv(jax.random.fold_in(jax.random.fold_in(key_of[7], part), 71), part),
        "block_table": draw_block_table(jax.random.fold_in(jax.random.fold_in(key_of[7], part), 71), part),
        "lengths": draw_lengths(jax.random.fold_in(jax.random.fold_in(key_of[7], part), 71), part),
        "join_step": jax.random.randint(part_keys[6], (1,), 1, STEPS).astype(jnp.int32),
    }


def attend(query_rows, head_keys, head_values, valid_mask, fresh_keys, fresh_values, fresh_valid):
    score_scale = 1.0 / math.sqrt(HD)
    highest = lax.Precision.HIGHEST

    def per_head(operands):
        rows_here, keys_here, values_here, new_keys, new_values = operands
        rows_wide = rows_here.astype(jnp.float32)
        cache_scores = jnp.einsum('sqd,ld->sql', rows_wide, keys_here.astype(jnp.float32), precision=highest) * score_scale
        cache_scores = jnp.where(valid_mask[None, None, :], cache_scores, -jnp.inf)
        fresh_scores = jnp.einsum('sqd,ud->squ', rows_wide, new_keys.astype(jnp.float32), precision=highest) * score_scale
        fresh_scores = jnp.where(fresh_valid[:, None, :], fresh_scores, -jnp.inf)
        row_max = jnp.maximum(lax.optimization_barrier(jnp.max(cache_scores, axis=-1)), lax.optimization_barrier(jnp.max(fresh_scores, axis=-1)))
        cache_weight = jnp.exp(cache_scores - row_max[..., None])
        fresh_weight = jnp.exp(fresh_scores - row_max[..., None])
        row_total = lax.optimization_barrier(jnp.sum(cache_weight, axis=-1)) + lax.optimization_barrier(jnp.sum(fresh_weight, axis=-1))
        cache_round = lax.optimization_barrier(cache_weight.astype(jnp.bfloat16)).astype(jnp.float32)
        fresh_round = lax.optimization_barrier(fresh_weight.astype(jnp.bfloat16)).astype(jnp.float32)
        summed = jnp.einsum('sql,ld->sqd', cache_round, values_here.astype(jnp.float32), precision=highest)
        summed = summed + jnp.einsum('squ,ud->sqd', fresh_round, new_values.astype(jnp.float32), precision=highest)
        return summed / row_total[..., None]
    answer = lax.map(per_head, (jnp.transpose(query_rows, (1, 0, 2, 3)), head_keys, head_values, jnp.transpose(fresh_keys, (1, 0, 2)), jnp.transpose(fresh_values, (1, 0, 2))))
    return jnp.transpose(answer, (1, 0, 2, 3)).reshape(STEPS, KVH * QPK, HD)

def reference(queries, new_kv, res_kv, prefill_kv, block_table, lengths, join_step):
    joined = join_step[0]
    step_ids = jnp.arange(STEPS, dtype=jnp.int32)
    earlier = step_ids[None, :] <= step_ids[:, None]
    answers = []
    for request in range(RES):
        valid_mask = jnp.arange(RES_LEN, dtype=jnp.int32) < lengths[request]
        query_rows = queries[:, request].reshape(STEPS, KVH, QPK, HD)
        head_keys = jnp.moveaxis(res_kv[0, request], 1, 0)
        head_values = jnp.moveaxis(res_kv[1, request], 1, 0)
        answers.append(attend(query_rows, head_keys, head_values, valid_mask, new_kv[0, :, request], new_kv[1, :, request], earlier))
    valid_mask = jnp.arange(LNEW, dtype=jnp.int32) < lengths[RES]
    query_rows = queries[:, RES].reshape(STEPS, KVH, QPK, HD)
    fresh_valid = earlier & (step_ids[None, :] >= joined)
    joining = attend(query_rows, prefill_kv[0], prefill_kv[1], valid_mask, new_kv[0, :, RES], new_kv[1, :, RES], fresh_valid)
    joining = jnp.where((step_ids >= joined)[:, None, None], joining, 0.0)
    attn_out = jnp.stack(answers + [joining], axis=1).astype(jnp.bfloat16)
    blocks = prefill_kv.reshape(2, KVH, NBLK, BLOCK, HD)
    new_cache = jnp.zeros_like(blocks).at[:, :, block_table].set(blocks).reshape(2, KVH, LNEW, HD)
    return (attn_out, new_cache)
```

```python
import functools
import math
import types

import jax
import jax.numpy as jnp
from jax import lax
from jax.experimental import pallas as pl
from jax.experimental.pallas import tpu as pltpu
from jax.sharding import PartitionSpec as P

very_low = -1e30
MESH = pl.DeviceIdType.MESH
NT = (((1,), (1,)), ((), ()))
NN = (((1,), (0,)), ((), ()))


def split_of(count):
    inner = 1
    for d in range(1, count + 1):
        if count % d == 0 and d * d <= count:
            inner = d
    return inner, count // inner


def named(groups):
    space = types.SimpleNamespace()
    for group in groups:
        for name, value in group.items():
            setattr(space, name, named([value]) if isinstance(value, dict) else value)
    return space


def kernel(seq_count, head_count, tree, *leaves):
    ref = named(jax.tree.unflatten(tree, leaves))
    q_hbm, fresh_hbm, prefill_hbm, res_hbm = ref.q_hbm, ref.fresh_hbm, ref.prefill_hbm, ref.res_hbm
    attn_out, cache_out = ref.attn_out, ref.cache_out
    table, lengths, joins = ref.table, ref.lengths, ref.joins
    arrived = ref.arrived
    inner, outer = split_of(seq_count)
    seq_index = lax.axis_index("seq")
    head_index = lax.axis_index("head")
    group = seq_index // inner

    def fold_back(g, p):
        return jnp.where(lax.rem(g, 2) == 0, p, inner - 1 - p)

    def member(g, p):
        return g * inner + fold_back(g, p)

    place_in = fold_back(group, lax.rem(seq_index, inner))
    step_count, request_count, group_size, head_dim = q_hbm.shape
    rows = step_count * group_size
    resident, res_rows = res_hbm.shape[1], res_hbm.shape[2]
    dev_blocks, block_len = prefill_hbm.shape[2], prefill_hbm.shape[3]
    senders = seq_count * head_count
    slot_count = senders * dev_blocks // seq_count
    per_dev = dev_blocks * block_len
    part, step_part = rows // inner, step_count // inner
    power = math.log2(math.e) / math.sqrt(head_dim)
    heads = [head_index] + [head_index ^ o for o in range(1, head_count)]
    held = ref.held
    staged = ref.staged

    barrier = pltpu.get_barrier_semaphore()

    def greet(**device):
        pl.semaphore_signal(barrier, inc=1, device_id=device, device_id_type=MESH)

    above, below = seq_index + 1 < seq_count, seq_index > 0
    pl.when(above)(lambda: greet(seq=seq_index + 1))
    pl.when(below)(lambda: greet(seq=seq_index - 1))
    for o in range(1, head_count):
        greet(head=heads[o])

    def tell(d):
        if d + 1 < seq_count:
            for sem, there, on, step in ((ref.above_sems, 1, below, -1), (ref.below_sems, -1, above, 1)):
                far = seq_index + there * d

                @pl.when((far >= 0) & (far < seq_count) & on)
                def _(sem=sem, step=step):
                    pl.semaphore_signal(
                        sem.at[d - 1], inc=1, device_id={"seq": seq_index + step}, device_id_type=MESH
                    )

    def learn(d):
        pl.when(seq_index + d < seq_count)(lambda: pl.semaphore_wait(ref.above_sems.at[d - 2], 1))
        pl.when(seq_index - d >= 0)(lambda: pl.semaphore_wait(ref.below_sems.at[d - 2], 1))
        tell(d)

    def local(source, target, sem):
        copy = pltpu.make_async_copy(source, target, sem)
        copy.start()
        return copy

    table_copy = local(ref.table_hbm, table, ref.table_sem)
    own_copy = local(prefill_hbm.at[:, head_index], held[0], ref.own_sem)
    q_copy = local(q_hbm, ref.q_buf, ref.q_sem)
    fresh_copy = local(fresh_hbm, ref.fresh_buf, ref.fresh_sem)
    length_copy = local(ref.lengths_hbm, lengths, ref.lengths_sem)
    join_copy = local(ref.joins_hbm, joins, ref.joins_sem)
    table_copy.wait()
    own_copy.wait()
    chunk = math.gcd(res_rows, 2048)
    chunks = res_rows // chunk
    res_copies = []
    for r in range(resident):
        for k in range(chunks):
            at = pl.ds(k * chunk, chunk)
            res_copies.append(local(res_hbm.at[:, r, at], ref.res_buf.at[:, r, at], ref.res_sems.at[r, k]))

    def remote(source, target, send_sem, recv_sem, **device):
        pltpu.make_async_remote_copy(
            src_ref=source, dst_ref=target, send_sem=send_sem, recv_sem=recv_sem, device_id=device, device_id_type=MESH
        ).start()

    def drain(part_ref, sem):
        pltpu.make_async_copy(part_ref, part_ref, sem).wait()

    def block_for(sender, shard):
        found = jnp.int32(0)
        for k in range(dev_blocks):
            hit = (table[sender * dev_blocks + k] // slot_count) == shard
            found = jnp.where(hit, k, found)
        return found

    def stage(o):
        sender = seq_index * head_count + heads[o]

        def body(z, _):
            found = block_for(sender, z)
            for c in range(2):
                staged[o][z, c] = held[o][c, found]
            return 0

        lax.fori_loop(0, seq_count, body, 0, unroll=seq_count <= 4)
        arrived[seq_index, heads[o]] = staged[o][seq_index]

    def forward(o, distances, inside=None, only=None):
        for d in distances:
            for peer in (seq_index - d, seq_index + d):

                wanted = (peer >= 0) & (peer < seq_count)
                if inside is not None:
                    wanted = wanted & ((peer // inner == group) == inside)

                if only is not None:
                    wanted = wanted & only

                @pl.when(wanted)
                def _(peer=peer):
                    target = arrived.at[seq_index, heads[o]]
                    remote(staged[o].at[peer], target, ref.block_send, ref.block_recv, seq=peer)

    def hand(o):
        remote(prefill_hbm.at[:, heads[o]], held[o], ref.held_send, ref.held_recv.at[o], head=heads[o])

    far_first = range(seq_count - 1, 0, -1)
    stage(0)
    pl.semaphore_wait(barrier, head_count - 1 + above.astype(jnp.int32) + below.astype(jnp.int32))
    tell(1)
    for o in range(1, min(3, head_count)):
        hand(o)
    forward(0, [1])

    def query_rows(r):
        wide = ref.q_buf[:, r].astype(jnp.float32).reshape(rows, head_dim)
        return wide.astype(jnp.bfloat16)

    def fold(carry, q, keys, values, valid):
        s = lax.dot_general(q, keys, NT, preferred_element_type=jnp.float32)
        s = jnp.where(valid, s, very_low)
        top = jnp.max(s, axis=1, keepdims=True)
        if carry is not None:
            top = jnp.maximum(carry[0], top)
        w = jnp.exp2((s - top) * power)
        l = jnp.sum(w, axis=1, keepdims=True)
        acc = lax.dot_general(w.astype(jnp.bfloat16), values, NN, preferred_element_type=jnp.float32)
        if carry is not None:
            keep = jnp.exp2((carry[0] - top) * power)
            l = carry[1] * keep + l
            acc = carry[2] * keep + acc
        return top, l, acc

    length_copy.wait()
    join_copy.wait()
    joined = joins[0, 0]
    q_copy.wait()
    fresh_copy.wait()

    when = lax.broadcasted_iota(jnp.int32, (rows, step_count), 0) // group_size
    which = lax.broadcasted_iota(jnp.int32, (rows, step_count), 1)

    def fold_fresh(carry, r, q):
        allowed = (which <= when) & (seq_index == seq_count - 1)
        if r >= resident:
            allowed = allowed & (which >= joined)
        return fold(carry, q, ref.fresh_buf[0, r], ref.fresh_buf[1, r], allowed)

    def attend_resident(r, between=lambda k: None):
        q = query_rows(r)
        limit = lengths[r] - seq_index * res_rows
        carry = None
        for k in range(chunks):
            res_copies[r * chunks + k].wait()
            at = pl.ds(k * chunk, chunk)
            valid = lax.broadcasted_iota(jnp.int32, (1, chunk), 1) < limit - k * chunk
            carry = fold(carry, q, ref.res_buf[0, r, at], ref.res_buf[1, r, at], valid)
            between(k)
        return fold_fresh(carry, r, q)

    lane = lax.broadcasted_iota(jnp.int32, (rows, rows), 1)

    class Batch:
        def __init__(self, refs, first, results, split):
            self.refs, self.first, self.count, self.split = refs, first, len(results), split and inner > 1
            self.size = part if self.split else rows
            self.mine = pl.ds(pl.multiple_of(place_in * part, part), part) if self.split else slice(0, rows)
            for k, (m, l, acc) in enumerate(results):
                refs.acc[k] = acc
                refs.sent[k] = acc.astype(jnp.bfloat16)
            self.pack(refs.stat, [r[:2] for r in results])
            for oi in range(1, inner):
                to_inner = lax.rem(place_in + oi, inner)
                peer, back = member(group, to_inner), inner - oi
                self.share(refs.stat, back, refs.stat_sems, peer)
                source = refs.sent
                if self.split:
                    source = source.at[:, pl.ds(pl.multiple_of(to_inner * part, part), part)]
                remote(source, refs.got.at[back], refs.got_sems.at[0], refs.got_sems.at[1], seq=peer)

        def pack(self, target, stats):
            count = stats[0][0].shape[0]
            packed = jnp.zeros((count, rows), jnp.float32)
            for k, (m, l) in enumerate(stats):
                packed = jnp.where(lane[0:count] == 2 * k, m, packed)
                packed = jnp.where(lane[0:count] == 2 * k + 1, l, packed)
            if count < rows:
                packed = jnp.concatenate([packed, jnp.zeros((rows - count, rows), jnp.float32)], axis=0)
            tile = jnp.transpose(packed)[0:8]
            target[0:8] = tile
            self.refs.stat_send[0 if target is self.refs.stat else 1] = tile

        def share(self, target, back, sems, peer):
            source = self.refs.stat_send.at[0 if target is self.refs.stat else 1]
            remote(source, target.at[pl.ds(8 * back, 8)], sems.at[0], sems.at[1], seq=peer)

        def columns(self, tiles, members):
            stats = tiles[0 : 8 * members]
            if 8 * members < rows:
                stats = jnp.concatenate([stats, jnp.zeros((rows - 8 * members, rows), jnp.float32)], axis=0)
            return jnp.transpose(stats)

        def combine(self, turned, members, k):
            maxima = [turned[:, 8 * z + 2 * k : 8 * z + 2 * k + 1] for z in members]
            totals = [turned[:, 8 * z + 2 * k + 1 : 8 * z + 2 * k + 2] for z in members]
            top = functools.reduce(jnp.maximum, maxima)
            factors = [jnp.exp2((m - top) * power) for m in maxima]
            return top, sum(f * t for f, t in zip(factors, totals)), factors

        def across(self):
            refs = self.refs
            if inner > 1:
                drain(refs.stat.at[pl.ds(8, 8 * (inner - 1))], refs.stat_sems.at[1])
            turned = self.columns(refs.stat, inner)
            if self.split:
                ref.turned[...] = turned
                turned = ref.turned[self.mine]
            if inner > 1:
                drain(refs.got.at[pl.ds(1, inner - 1)], refs.got_sems.at[1])
            stats = []
            for k in range(self.count):
                top, total, factors = self.combine(turned, range(inner), k)
                summed = refs.acc[k, self.mine] * factors[0]
                for oi in range(1, inner):
                    summed = summed + refs.got[oi, k].astype(jnp.float32) * factors[oi]
                refs.level[0, k] = (summed / total).astype(jnp.bfloat16)
                stats.append((top, total))
            self.pack(refs.group_stat, stats)
            for og in range(1, outer):
                peer = member(lax.rem(group + og, outer), place_in)
                self.share(refs.group_stat, outer - og, refs.group_sems, peer)
                target = refs.level.at[outer - og]
                remote(refs.level.at[0], target, refs.level_sems.at[0], refs.level_sems.at[1], seq=peer)

        def finish(self):
            refs, level = self.refs, self.refs.level
            drain(refs.group_stat.at[pl.ds(8, 8 * (outer - 1))], refs.group_sems.at[1])
            turned = self.columns(refs.group_stat, outer)[0 : self.size]
            drain(level.at[pl.ds(1, outer - 1)], refs.level_sems.at[1])
            offset = place_in * step_part if self.split else 0
            steps = pl.ds(offset, self.size // group_size)
            for k in range(self.count):
                _, whole, factors = self.combine(turned, range(outer), k)
                result = jnp.zeros((self.size, head_dim), jnp.float32)
                for g in range(outer):
                    total = turned[:, 8 * g + 2 * k + 1 : 8 * g + 2 * k + 2]
                    result = result + level[g, k].astype(jnp.float32) * (factors[g] * total / whole)
                if self.first + k >= resident:
                    at = lax.broadcasted_iota(jnp.int32, (self.size, head_dim), 0) // group_size
                    result = jnp.where(at + offset >= joined, result, 0.0)
                result = result.reshape(self.size // group_size, group_size, head_dim)
                attn_out[steps, self.first + k] = result.astype(jnp.bfloat16)
            if self.split:
                piece = attn_out.at[steps, pl.ds(self.first, self.count)]
                for oi in range(1, inner):
                    peer = member(group, lax.rem(place_in + oi, inner))
                    remote(piece, piece, refs.final_sems.at[0], refs.final_sems.at[1], seq=peer)

        def close(self):
            refs = self.refs
            if self.split:
                others = attn_out.at[pl.ds(0, step_part * (inner - 1)), pl.ds(self.first, self.count)]
                drain(others, refs.final_sems.at[1])
                drain(others, refs.final_sems.at[0])
            if inner > 1:
                drain(refs.got.at[pl.ds(1, inner - 1)], refs.got_sems.at[0])
                drain(refs.stat.at[pl.ds(8, 8 * (inner - 1))], refs.stat_sems.at[0])
            drain(refs.group_stat.at[pl.ds(8, 8 * (outer - 1))], refs.group_sems.at[0])
            drain(refs.level.at[pl.ds(1, outer - 1)], refs.level_sems.at[0])

    def take(o):
        drain(held[o], ref.held_recv.at[o])
        stage(o)

    def between(k):
        if k == 0 and seq_count > 2:
            learn(2)
            forward(0, [2])

    results = [attend_resident(0, between)]
    for o in range(3, head_count):
        hand(o)
    for d in range(3, seq_count):
        learn(d)
        forward(0, [d])
    take(1)
    forward(1, far_first, False)
    results += [attend_resident(r) for r in range(1, resident)]
    batch_a = Batch(ref.batch_a, 0, results, True)
    forward(1, far_first, True)
    edge = (seq_index == 0) | (seq_index == seq_count - 1)

    q = query_rows(resident)

    def attend_new(carry, o):
        keys = held[o][0].reshape(per_dev, head_dim)
        values = held[o][1].reshape(per_dev, head_dim)
        base = (seq_index * head_count + heads[o]) * per_dev
        valid = lax.broadcasted_iota(jnp.int32, (1, per_dev), 1) + base < lengths[resident]
        return fold(carry, q, keys, values, valid)

    carry = fold_fresh(None, resident, q)
    for o in range(2):
        carry = attend_new(carry, o)
    for o in range(2, head_count - 1):
        take(o)
        forward(o, far_first, False, edge)
        carry = attend_new(carry, o)
    sources = ref.sources

    def locate(s, _):
        slot = jnp.int32(0)
        for k in range(dev_blocks):
            here = table[s * dev_blocks + k]
            slot = jnp.where((here // slot_count) == seq_index, here, slot)
        ref.slot_of[s] = slot - seq_index * slot_count
        return 0

    lax.fori_loop(0, senders, locate, 0)

    def source_for(j, _):
        def look(s, found):
            return jnp.where(ref.slot_of[s] == j, s, found)

        sources[j] = lax.fori_loop(0, senders, look, jnp.int32(0), unroll=math.gcd(senders, 16))
        return 0

    lax.fori_loop(0, slot_count, source_for, 0)

    batch_a.across()
    last = range(max(head_count - 1, 2), head_count)
    for o in range(2, head_count - 1):
        forward(o, far_first, False, jnp.logical_not(edge))
    for o in last:
        take(o)
        carry = attend_new(carry, o)
    batch_b = Batch(ref.batch_b, resident, [carry], False)
    for o in last:
        forward(o, far_first, False)
    for o in range(2, head_count - 1):
        forward(o, far_first, True)
    batch_b.across()
    for o in last:
        forward(o, far_first, True)
    batch_a.finish()
    batch_b.finish()

    part_ref = arrived.at[pl.ds(0, seq_count - 1)]
    drain(part_ref, ref.block_recv)

    def place(j, _):
        source = sources[j]
        at = pl.ds(pl.multiple_of(j * block_len, block_len), block_len)
        for c in range(2):
            cache_out[c, 0, at] = arrived[source // head_count, lax.rem(source, head_count), c]
        return 0

    lax.fori_loop(0, slot_count, place, 0, unroll=math.gcd(slot_count, 4))
    batch_a.close()
    batch_b.close()
    drain(part_ref, ref.block_send)
    for o in range(1, head_count):
        drain(held[o], ref.held_send)


def store_kernel(attn, cache, attn_out, cache_out, sems):
    copies = [pltpu.make_async_copy(cache.at[c], cache_out.at[c], sems.at[c]) for c in range(2)]
    copies.append(pltpu.make_async_copy(attn, attn_out, sems.at[2]))
    for copy in copies:
        copy.start()
    for copy in copies:
        copy.wait()


def per_device(seq_count, head_count, queries, new_kv, res_kv, prefill_kv, block_table, lengths, join_step):
    step_count, request_count, group_size, head_dim = queries.shape
    rows = step_count * group_size
    resident, res_rows = res_kv.shape[1], res_kv.shape[2]
    head_total, new_rows = prefill_kv.shape[1], prefill_kv.shape[2]
    senders = seq_count * head_count
    dev_blocks = block_table.shape[0] // senders
    block_len = new_rows // dev_blocks
    if dev_blocks != seq_count or resident > 3 or head_total != head_count:
        raise ValueError("unsupported sizes")
    if head_count & (head_count - 1) or head_count < 2 or seq_count < 2 or 8 * seq_count > rows or rows != head_dim:
        raise ValueError("unsupported sizes")
    inner, outer = split_of(seq_count)
    part = rows // inner
    slot_count = block_table.shape[0] // seq_count
    fresh = jnp.transpose(new_kv[:, :, :, 0], (0, 2, 1, 3))
    prefill = prefill_kv.reshape(2, head_total, dev_blocks, block_len, head_dim)
    bf16, f32, i32 = jnp.bfloat16, jnp.float32, jnp.int32
    vmem = pl.BlockSpec(memory_space=pltpu.VMEM)
    hbm = pl.BlockSpec(memory_space=pltpu.HBM)
    chunks = res_rows // math.gcd(res_rows, 2048)
    dma = pltpu.SemaphoreType.DMA
    def vm(dtype, *shape):
        return pltpu.VMEM(shape, dtype)

    def batch(count, size):
        return dict(
            acc=vm(f32, count, rows, head_dim),
            sent=vm(bf16, count, rows, head_dim),
            got=vm(bf16, inner, count, size, head_dim),
            level=vm(bf16, outer, count, size, head_dim),
            stat_send=vm(f32, 2, 8, rows),
            stat=vm(f32, 8 * inner, rows),
            group_stat=vm(f32, 8 * outer, rows),
            stat_sems=dma((2,)),
            group_sems=dma((2,)),
            got_sems=dma((2,)),
            level_sems=dma((2,)),
            final_sems=dma((2,)),
        )

    regular = pltpu.SemaphoreType.REGULAR((max(seq_count - 2, 1),))
    scratch = dict(
        q_buf=vm(bf16, *queries.shape),
        fresh_buf=vm(bf16, *fresh.shape),
        res_buf=vm(bf16, 2, resident, res_rows, head_dim),
        table=pltpu.SMEM(block_table.shape, i32),
        lengths=pltpu.SMEM(lengths.shape, i32),
        joins=pltpu.SMEM((1, 1), i32),
        slot_of=pltpu.SMEM((senders,), i32),
        sources=pltpu.SMEM((slot_count,), i32),
        arrived=vm(bf16, seq_count, head_count, 2, block_len, head_dim),
        turned=vm(f32, rows, rows),
        own_sem=dma,
        table_sem=dma,
        q_sem=dma,
        fresh_sem=dma,
        lengths_sem=dma,
        joins_sem=dma,
        res_sems=dma((resident, chunks)),
        block_send=dma,
        block_recv=dma,
        held_send=dma,
        held_recv=dma((head_count,)),
        above_sems=regular,
        below_sems=regular,
        held=[vm(bf16, 2, dev_blocks, block_len, head_dim) for _ in range(head_count)],
        staged=[vm(bf16, seq_count, 2, block_len, head_dim) for _ in range(head_count)],
        batch_a=batch(resident, part),
        batch_b=batch(1, rows),
    )
    inputs = dict(
        q_hbm=queries,
        fresh_hbm=fresh,
        prefill_hbm=prefill,
        table_hbm=block_table,
        lengths_hbm=lengths,
        joins_hbm=join_step.reshape(1, 1),
        res_hbm=res_kv.reshape(2, resident, res_rows, head_dim),
    )
    outputs = dict(
        attn_out=pltpu.VMEM(queries.shape, bf16),
        cache_out=pltpu.VMEM((2, 1, slot_count * block_len, head_dim), bf16),
    )
    operands = jax.tree.leaves(inputs)
    tree = jax.tree.structure((inputs, outputs, scratch))
    out_bytes = 2 * (queries.size + 2 * slot_count * block_len * head_dim)
    attn, cache = pl.pallas_call(
        functools.partial(kernel, seq_count, head_count, tree),
        out_shape=tuple(jax.tree.leaves(outputs)),
        in_specs=[hbm] * len(operands),
        out_specs=(vmem, vmem),
        scratch_shapes=jax.tree.leaves(scratch),
        compiler_params=pltpu.CompilerParams(
            collective_id=0, has_side_effects=True, vmem_limit_bytes=62 * 2**20 - 3 * out_bytes
        ),
    )(*operands)
    return pl.pallas_call(
        store_kernel,
        out_shape=(
            jax.ShapeDtypeStruct(attn.shape, bf16),
            jax.ShapeDtypeStruct(cache.shape, bf16),
        ),
        in_specs=[vmem, vmem],
        out_specs=(hbm, hbm),
        scratch_shapes=[dma((3,))],
        compiler_params=pltpu.CompilerParams(vmem_limit_bytes=2**20),
    )(pltpu.with_memory_space_constraint(attn, pltpu.VMEM), pltpu.with_memory_space_constraint(cache, pltpu.VMEM))


def solution(mesh):
    in_specs = (
        P("groups", None, "head", None),
        P("groups", None, None, "head", None),
        P("groups", None, "seq", "head", None),
        P("groups", None, ("seq", "head"), None),
        P("groups"),
        P("groups"),
        P("groups"),
    )
    out_specs = (P("groups", None, "head", None), P("groups", "head", "seq", None))
    body = functools.partial(per_device, mesh.shape["seq"], mesh.shape["head"])
    return jax.shard_map(body, mesh=mesh, in_specs=in_specs, out_specs=out_specs, check_vma=False)
```

```python
import functools
import math
import types

import jax
import jax.numpy as jnp
from jax import lax
from jax.experimental import pallas as pl
from jax.experimental.pallas import tpu as pltpu
from jax.sharding import PartitionSpec as P

very_low = -1e30
MESH = pl.DeviceIdType.MESH
NT = (((1,), (1,)), ((), ()))
NN = (((1,), (0,)), ((), ()))


def split_of(count):
    inner = 1
    for d in range(1, count + 1):
        if count % d == 0 and d * d <= count:
            inner = d
    return inner, count // inner


def named(groups):
    space = types.SimpleNamespace()
    for group in groups:
        for name, value in group.items():
            setattr(space, name, named([value]) if isinstance(value, dict) else value)
    return space


def kernel(seq_count, head_count, tree, *leaves):
    ref = named(jax.tree.unflatten(tree, leaves))
    q_hbm, fresh_hbm, prefill_hbm, res_hbm = ref.q_hbm, ref.fresh_hbm, ref.prefill_hbm, ref.res_hbm
    attn_out, cache_out = ref.attn_out, ref.cache_out
    table, lengths, joins = ref.table, ref.lengths, ref.joins
    arrived = ref.arrived
    inner, outer = split_of(seq_count)
    seq_index = lax.axis_index("seq")
    head_index = lax.axis_index("head")
    group = seq_index // inner

    def fold_back(g, p):
        return jnp.where(lax.rem(g, 2) == 0, p, inner - 1 - p)

    def member(g, p):
        return g * inner + fold_back(g, p)

    place_in = fold_back(group, lax.rem(seq_index, inner))
    step_count, request_count, group_size, head_dim = q_hbm.shape
    rows = step_count * group_size
    resident, res_rows = res_hbm.shape[1], res_hbm.shape[2]
    dev_blocks, block_len = prefill_hbm.shape[2], prefill_hbm.shape[3]
    senders = seq_count * head_count
    slot_count = senders * dev_blocks // seq_count
    per_dev = dev_blocks * block_len
    part, step_part = rows // inner, step_count // inner
    power = math.log2(math.e) / math.sqrt(head_dim)
    heads = [head_index] + [head_index ^ o for o in range(1, head_count)]
    held = ref.held
    staged = ref.staged

    barrier = pltpu.get_barrier_semaphore()

    def greet(**device):
        pl.semaphore_signal(barrier, inc=1, device_id=device, device_id_type=MESH)

    above, below = seq_index + 1 < seq_count, seq_index > 0
    pl.when(above)(lambda: greet(seq=seq_index + 1))
    pl.when(below)(lambda: greet(seq=seq_index - 1))
    for o in range(1, head_count):
        greet(head=heads[o])

    def tell(d):
        if d + 1 < seq_count:
            for sem, there, on, step in ((ref.above_sems, 1, below, -1), (ref.below_sems, -1, above, 1)):
                far = seq_index + there * d

                @pl.when((far >= 0) & (far < seq_count) & on)
                def _(sem=sem, step=step):
                    pl.semaphore_signal(
                        sem.at[d - 1], inc=1, device_id={"seq": seq_index + step}, device_id_type=MESH
                    )

    def learn(d):
        pl.when(seq_index + d < seq_count)(lambda: pl.semaphore_wait(ref.above_sems.at[d - 2], 1))
        pl.when(seq_index - d >= 0)(lambda: pl.semaphore_wait(ref.below_sems.at[d - 2], 1))
        tell(d)

    def local(source, target, sem):
        copy = pltpu.make_async_copy(source, target, sem)
        copy.start()
        return copy

    table_copy = local(ref.table_hbm, table, ref.table_sem)
    own_copy = local(prefill_hbm.at[:, head_index], held[0], ref.own_sem)
    all_copy = local(prefill_hbm, ref.all_buf, ref.all_sem)
    q_copy = local(q_hbm, ref.q_buf, ref.q_sem)
    fresh_copy = local(fresh_hbm, ref.fresh_buf, ref.fresh_sem)
    length_copy = local(ref.lengths_hbm, lengths, ref.lengths_sem)
    join_copy = local(ref.joins_hbm, joins, ref.joins_sem)
    table_copy.wait()
    own_copy.wait()
    chunk = math.gcd(res_rows, 2048)
    chunks = res_rows // chunk
    res_copies = []
    for r in range(resident):
        for k in range(chunks):
            at = pl.ds(k * chunk, chunk)
            res_copies.append(local(res_hbm.at[:, r, at], ref.res_buf.at[:, r, at], ref.res_sems.at[r, k]))

    def remote(source, target, send_sem, recv_sem, **device):
        pltpu.make_async_remote_copy(
            src_ref=source, dst_ref=target, send_sem=send_sem, recv_sem=recv_sem, device_id=device, device_id_type=MESH
        ).start()

    def drain(part_ref, sem):
        pltpu.make_async_copy(part_ref, part_ref, sem).wait()

    def block_for(sender, shard):
        found = jnp.int32(0)
        for k in range(dev_blocks):
            hit = (table[sender * dev_blocks + k] // slot_count) == shard
            found = jnp.where(hit, k, found)
        return found

    def stage(o):
        sender = seq_index * head_count + heads[o]

        def body(z, _):
            found = block_for(sender, z)
            for c in range(2):
                staged[o][z, c] = held[o][c, found]
            return 0

        lax.fori_loop(0, seq_count, body, 0, unroll=seq_count <= 4)
        arrived[seq_index, heads[o]] = staged[o][seq_index]

    def forward(o, distances, inside=None, only=None):
        for d in distances:
            for peer in (seq_index - d, seq_index + d):

                wanted = (peer >= 0) & (peer < seq_count)
                if inside is not None:
                    wanted = wanted & ((peer // inner == group) == inside)

                if only is not None:
                    wanted = wanted & only

                @pl.when(wanted)
                def _(peer=peer):
                    target = arrived.at[seq_index, heads[o]]
                    remote(staged[o].at[peer], target, ref.block_send, ref.block_recv, seq=peer)

    def hand(o):
        remote(ref.all_buf.at[:, heads[o]], held[o], ref.held_send, ref.held_recv.at[o], head=heads[o])

    far_first = range(seq_count - 1, 0, -1)
    stage(0)
    all_copy.wait()
    pl.semaphore_wait(barrier, head_count - 1 + above.astype(jnp.int32) + below.astype(jnp.int32))
    tell(1)
    for o in range(1, head_count):
        hand(o)
    forward(0, [1])

    def query_rows(r):
        wide = ref.q_buf[:, r].astype(jnp.float32).reshape(rows, head_dim)
        return wide.astype(jnp.bfloat16)

    def fold(carry, q, keys, values, valid):
        s = lax.dot_general(q, keys, NT, preferred_element_type=jnp.float32)
        s = jnp.where(valid, s, very_low)
        top = jnp.max(s, axis=1, keepdims=True)
        if carry is not None:
            top = jnp.maximum(carry[0], top)
        w = jnp.exp2((s - top) * power)
        l = jnp.sum(w, axis=1, keepdims=True)
        acc = lax.dot_general(w.astype(jnp.bfloat16), values, NN, preferred_element_type=jnp.float32)
        if carry is not None:
            keep = jnp.exp2((carry[0] - top) * power)
            l = carry[1] * keep + l
            acc = carry[2] * keep + acc
        return top, l, acc

    length_copy.wait()
    join_copy.wait()
    joined = joins[0, 0]
    q_copy.wait()
    fresh_copy.wait()

    when = lax.broadcasted_iota(jnp.int32, (rows, step_count), 0) // group_size
    which = lax.broadcasted_iota(jnp.int32, (rows, step_count), 1)

    def fold_fresh(carry, r, q):
        allowed = (which <= when) & (seq_index == seq_count - 1)
        if r >= resident:
            allowed = allowed & (which >= joined)
        return fold(carry, q, ref.fresh_buf[0, r], ref.fresh_buf[1, r], allowed)

    def attend_resident(r, between=lambda k: None):
        q = query_rows(r)
        limit = lengths[r] - seq_index * res_rows
        carry = None
        for k in range(chunks):
            res_copies[r * chunks + k].wait()
            at = pl.ds(k * chunk, chunk)
            valid = lax.broadcasted_iota(jnp.int32, (1, chunk), 1) < limit - k * chunk
            carry = fold(carry, q, ref.res_buf[0, r, at], ref.res_buf[1, r, at], valid)
            between(k)
        return fold_fresh(carry, r, q)

    lane = lax.broadcasted_iota(jnp.int32, (rows, rows), 1)

    class Batch:
        def __init__(self, refs, first, results, split):
            self.refs, self.first, self.count, self.split = refs, first, len(results), split and inner > 1
            self.size = part if self.split else rows
            self.mine = pl.ds(pl.multiple_of(place_in * part, part), part) if self.split else slice(0, rows)
            for k, (m, l, acc) in enumerate(results):
                refs.acc[k] = acc
                refs.sent[k] = acc.astype(jnp.bfloat16)
            self.pack(refs.stat, [r[:2] for r in results])
            for oi in range(1, inner):
                to_inner = lax.rem(place_in + oi, inner)
                peer, back = member(group, to_inner), inner - oi
                self.share(refs.stat, back, refs.stat_sems, peer)
                source = refs.sent
                if self.split:
                    source = source.at[:, pl.ds(pl.multiple_of(to_inner * part, part), part)]
                remote(source, refs.got.at[back], refs.got_sems.at[0], refs.got_sems.at[1], seq=peer)

        def pack(self, target, stats):
            count = stats[0][0].shape[0]
            packed = jnp.zeros((count, rows), jnp.float32)
            for k, (m, l) in enumerate(stats):
                packed = jnp.where(lane[0:count] == 2 * k, m, packed)
                packed = jnp.where(lane[0:count] == 2 * k + 1, l, packed)
            if count < rows:
                packed = jnp.concatenate([packed, jnp.zeros((rows - count, rows), jnp.float32)], axis=0)
            tile = jnp.transpose(packed)[0:8]
            target[0:8] = tile
            self.refs.stat_send[0 if target is self.refs.stat else 1] = tile

        def share(self, target, back, sems, peer):
            source = self.refs.stat_send.at[0 if target is self.refs.stat else 1]
            remote(source.at[pl.ds(0, 2 * self.count)], target.at[pl.ds(8 * back, 2 * self.count)], sems.at[0], sems.at[1], seq=peer)

        def columns(self, tiles, members):
            stats = tiles[0 : 8 * members]
            if 8 * members < rows:
                stats = jnp.concatenate([stats, jnp.zeros((rows - 8 * members, rows), jnp.float32)], axis=0)
            return jnp.transpose(stats)

        def combine(self, turned, members, k):
            maxima = [turned[:, 8 * z + 2 * k : 8 * z + 2 * k + 1] for z in members]
            totals = [turned[:, 8 * z + 2 * k + 1 : 8 * z + 2 * k + 2] for z in members]
            top = functools.reduce(jnp.maximum, maxima)
            factors = [jnp.exp2((m - top) * power) for m in maxima]
            return top, sum(f * t for f, t in zip(factors, totals)), factors

        def across(self):
            refs = self.refs
            if inner > 1:
                drain(refs.stat.at[pl.ds(0, 2 * self.count * (inner - 1))], refs.stat_sems.at[1])
            turned = self.columns(refs.stat, inner)
            if self.split:
                ref.turned[...] = turned
                turned = ref.turned[self.mine]
            if inner > 1:
                drain(refs.got.at[pl.ds(1, inner - 1)], refs.got_sems.at[1])
            stats = []
            for k in range(self.count):
                top, total, factors = self.combine(turned, range(inner), k)
                summed = refs.acc[k, self.mine] * factors[0]
                for oi in range(1, inner):
                    summed = summed + refs.got[oi, k].astype(jnp.float32) * factors[oi]
                refs.level[0, k] = (summed / total).astype(jnp.bfloat16)
                stats.append((top, total))
            self.pack(refs.group_stat, stats)
            for og in range(1, outer):
                peer = member(lax.rem(group + og, outer), place_in)
                self.share(refs.group_stat, outer - og, refs.group_sems, peer)
                target = refs.level.at[outer - og]
                remote(refs.level.at[0], target, refs.level_sems.at[0], refs.level_sems.at[1], seq=peer)

        def finish(self):
            refs, level = self.refs, self.refs.level
            drain(refs.group_stat.at[pl.ds(0, 2 * self.count * (outer - 1))], refs.group_sems.at[1])
            turned = self.columns(refs.group_stat, outer)[0 : self.size]
            drain(level.at[pl.ds(1, outer - 1)], refs.level_sems.at[1])
            offset = place_in * step_part if self.split else 0
            steps = pl.ds(offset, self.size // group_size)
            for k in range(self.count):
                _, whole, factors = self.combine(turned, range(outer), k)
                result = jnp.zeros((self.size, head_dim), jnp.float32)
                for g in range(outer):
                    total = turned[:, 8 * g + 2 * k + 1 : 8 * g + 2 * k + 2]
                    result = result + level[g, k].astype(jnp.float32) * (factors[g] * total / whole)
                if self.first + k >= resident:
                    at = lax.broadcasted_iota(jnp.int32, (self.size, head_dim), 0) // group_size
                    result = jnp.where(at + offset >= joined, result, 0.0)
                result = result.reshape(self.size // group_size, group_size, head_dim)
                attn_out[steps, self.first + k] = result.astype(jnp.bfloat16)
            if self.split:
                piece = attn_out.at[steps, pl.ds(self.first, self.count)]
                for oi in range(1, inner):
                    peer = member(group, lax.rem(place_in + oi, inner))
                    remote(piece, piece, refs.final_sems.at[0], refs.final_sems.at[1], seq=peer)

        def close(self):
            refs = self.refs
            if self.split:
                others = attn_out.at[pl.ds(0, step_part * (inner - 1)), pl.ds(self.first, self.count)]
                drain(others, refs.final_sems.at[1])
                drain(others, refs.final_sems.at[0])
            if inner > 1:
                drain(refs.got.at[pl.ds(1, inner - 1)], refs.got_sems.at[0])
                drain(refs.stat.at[pl.ds(0, 2 * self.count * (inner - 1))], refs.stat_sems.at[0])
            drain(refs.group_stat.at[pl.ds(0, 2 * self.count * (outer - 1))], refs.group_sems.at[0])
            drain(refs.level.at[pl.ds(1, outer - 1)], refs.level_sems.at[0])

    def take(o):
        drain(held[o], ref.held_recv.at[o])
        stage(o)

    def between(k):
        if k == 0 and seq_count > 2:
            learn(2)
            forward(0, [2])

    results = [attend_resident(0, between)]
    for d in range(3, seq_count):
        learn(d)
        forward(0, [d])
    take(1)
    forward(1, far_first, False)
    results += [attend_resident(r) for r in range(1, resident)]
    batch_a = Batch(ref.batch_a, 0, results, True)
    forward(1, far_first, True)
    edge = (seq_index == 0) | (seq_index == seq_count - 1)

    q = query_rows(resident)

    def attend_new(carry, o):
        keys = held[o][0].reshape(per_dev, head_dim)
        values = held[o][1].reshape(per_dev, head_dim)
        base = (seq_index * head_count + heads[o]) * per_dev
        valid = lax.broadcasted_iota(jnp.int32, (1, per_dev), 1) + base < lengths[resident]
        return fold(carry, q, keys, values, valid)

    carry = fold_fresh(None, resident, q)
    for o in range(2):
        carry = attend_new(carry, o)
    for o in range(2, head_count - 1):
        take(o)
        forward(o, far_first, False, edge)
        carry = attend_new(carry, o)
    sources = ref.sources

    def locate(s, _):
        slot = jnp.int32(0)
        for k in range(dev_blocks):
            here = table[s * dev_blocks + k]
            slot = jnp.where((here // slot_count) == seq_index, here, slot)
        ref.slot_of[s] = slot - seq_index * slot_count
        return 0

    lax.fori_loop(0, senders, locate, 0)

    def source_for(j, _):
        def look(s, found):
            return jnp.where(ref.slot_of[s] == j, s, found)

        sources[j] = lax.fori_loop(0, senders, look, jnp.int32(0), unroll=math.gcd(senders, 16))
        return 0

    lax.fori_loop(0, slot_count, source_for, 0)

    batch_a.across()
    last = range(max(head_count - 1, 2), head_count)
    for o in range(2, head_count - 1):
        forward(o, far_first, False, jnp.logical_not(edge))
    for o in last:
        take(o)
        carry = attend_new(carry, o)
    batch_b = Batch(ref.batch_b, resident, [carry], False)
    for o in last:
        forward(o, far_first, False)
    for o in range(2, head_count - 1):
        forward(o, far_first, True)
    batch_b.across()
    for o in last:
        forward(o, far_first, True)
    batch_a.finish()
    batch_b.finish()

    part_ref = arrived.at[pl.ds(0, seq_count - 1)]
    drain(part_ref, ref.block_recv)

    def place(j, _):
        source = sources[j]
        at = pl.ds(pl.multiple_of(j * block_len, block_len), block_len)
        for c in range(2):
            cache_out[c, 0, at] = arrived[source // head_count, lax.rem(source, head_count), c]
        return 0

    lax.fori_loop(0, slot_count, place, 0, unroll=math.gcd(slot_count, 4))
    batch_a.close()
    batch_b.close()
    drain(part_ref, ref.block_send)
    for o in range(1, head_count):
        drain(held[o], ref.held_send)


def store_kernel(attn, cache, attn_out, cache_out, sems):
    copies = [pltpu.make_async_copy(cache.at[c], cache_out.at[c], sems.at[c]) for c in range(2)]
    copies.append(pltpu.make_async_copy(attn, attn_out, sems.at[2]))
    for copy in copies:
        copy.start()
    for copy in copies:
        copy.wait()


def per_device(seq_count, head_count, queries, new_kv, res_kv, prefill_kv, block_table, lengths, join_step):
    step_count, request_count, group_size, head_dim = queries.shape
    rows = step_count * group_size
    resident, res_rows = res_kv.shape[1], res_kv.shape[2]
    head_total, new_rows = prefill_kv.shape[1], prefill_kv.shape[2]
    senders = seq_count * head_count
    dev_blocks = block_table.shape[0] // senders
    block_len = new_rows // dev_blocks
    if dev_blocks != seq_count or resident > 3 or head_total != head_count:
        raise ValueError("unsupported sizes")
    if head_count & (head_count - 1) or head_count < 2 or seq_count < 2 or 8 * seq_count > rows or rows != head_dim:
        raise ValueError("unsupported sizes")
    inner, outer = split_of(seq_count)
    part = rows // inner
    slot_count = block_table.shape[0] // seq_count
    fresh = jnp.transpose(new_kv[:, :, :, 0], (0, 2, 1, 3))
    prefill = prefill_kv.reshape(2, head_total, dev_blocks, block_len, head_dim)
    bf16, f32, i32 = jnp.bfloat16, jnp.float32, jnp.int32
    vmem = pl.BlockSpec(memory_space=pltpu.VMEM)
    hbm = pl.BlockSpec(memory_space=pltpu.HBM)
    chunks = res_rows // math.gcd(res_rows, 2048)
    dma = pltpu.SemaphoreType.DMA
    def vm(dtype, *shape):
        return pltpu.VMEM(shape, dtype)

    def batch(count, size):
        return dict(
            acc=vm(f32, count, rows, head_dim),
            sent=vm(bf16, count, rows, head_dim),
            got=vm(bf16, inner, count, size, head_dim),
            level=vm(bf16, outer, count, size, head_dim),
            stat_send=vm(f32, 2, 8, rows),
            stat=vm(f32, 8 * inner, rows),
            group_stat=vm(f32, 8 * outer, rows),
            stat_sems=dma((2,)),
            group_sems=dma((2,)),
            got_sems=dma((2,)),
            level_sems=dma((2,)),
            final_sems=dma((2,)),
        )

    regular = pltpu.SemaphoreType.REGULAR((max(seq_count - 2, 1),))
    scratch = dict(
        q_buf=vm(bf16, *queries.shape),
        fresh_buf=vm(bf16, *fresh.shape),
        res_buf=vm(bf16, 2, resident, res_rows, head_dim),
        table=pltpu.SMEM(block_table.shape, i32),
        lengths=pltpu.SMEM(lengths.shape, i32),
        joins=pltpu.SMEM((1, 1), i32),
        slot_of=pltpu.SMEM((senders,), i32),
        sources=pltpu.SMEM((slot_count,), i32),
        arrived=vm(bf16, seq_count, head_count, 2, block_len, head_dim),
        turned=vm(f32, rows, rows),
        own_sem=dma,
        all_sem=dma,
        all_buf=vm(bf16, *prefill.shape),
        table_sem=dma,
        q_sem=dma,
        fresh_sem=dma,
        lengths_sem=dma,
        joins_sem=dma,
        res_sems=dma((resident, chunks)),
        block_send=dma,
        block_recv=dma,
        held_send=dma,
        held_recv=dma((head_count,)),
        above_sems=regular,
        below_sems=regular,
        held=[vm(bf16, 2, dev_blocks, block_len, head_dim) for _ in range(head_count)],
        staged=[vm(bf16, seq_count, 2, block_len, head_dim) for _ in range(head_count)],
        batch_a=batch(resident, part),
        batch_b=batch(1, rows),
    )
    inputs = dict(
        q_hbm=queries,
        fresh_hbm=fresh,
        prefill_hbm=prefill,
        table_hbm=block_table,
        lengths_hbm=lengths,
        joins_hbm=join_step.reshape(1, 1),
        res_hbm=res_kv.reshape(2, resident, res_rows, head_dim),
    )
    outputs = dict(
        attn_out=pltpu.VMEM(queries.shape, bf16),
        cache_out=pltpu.VMEM((2, 1, slot_count * block_len, head_dim), bf16),
    )
    operands = jax.tree.leaves(inputs)
    tree = jax.tree.structure((inputs, outputs, scratch))
    out_bytes = 2 * (queries.size + 2 * slot_count * block_len * head_dim)
    attn, cache = pl.pallas_call(
        functools.partial(kernel, seq_count, head_count, tree),
        out_shape=tuple(jax.tree.leaves(outputs)),
        in_specs=[hbm] * len(operands),
        out_specs=(vmem, vmem),
        scratch_shapes=jax.tree.leaves(scratch),
        compiler_params=pltpu.CompilerParams(
            collective_id=0, has_side_effects=True, vmem_limit_bytes=62 * 2**20 - 3 * out_bytes
        ),
    )(*operands)
    return pl.pallas_call(
        store_kernel,
        out_shape=(
            jax.ShapeDtypeStruct(attn.shape, bf16),
            jax.ShapeDtypeStruct(cache.shape, bf16),
        ),
        in_specs=[vmem, vmem],
        out_specs=(hbm, hbm),
        scratch_shapes=[dma((3,))],
        compiler_params=pltpu.CompilerParams(vmem_limit_bytes=2**20),
    )(pltpu.with_memory_space_constraint(attn, pltpu.VMEM), pltpu.with_memory_space_constraint(cache, pltpu.VMEM))


def solution(mesh):
    in_specs = (
        P("groups", None, "head", None),
        P("groups", None, None, "head", None),
        P("groups", None, "seq", "head", None),
        P("groups", None, ("seq", "head"), None),
        P("groups"),
        P("groups"),
        P("groups"),
    )
    out_specs = (P("groups", None, "head", None), P("groups", "head", "seq", None))
    body = functools.partial(per_device, mesh.shape["seq"], mesh.shape["head"])
    return jax.shard_map(body, mesh=mesh, in_specs=in_specs, out_specs=out_specs, check_vma=False)
```

```python
import functools
import math
import types

import jax
import jax.numpy as jnp
from jax import lax
from jax.experimental import pallas as pl
from jax.experimental.pallas import tpu as pltpu
from jax.sharding import PartitionSpec as P

very_low = -1e30
MESH = pl.DeviceIdType.MESH
NT = (((1,), (1,)), ((), ()))
NN = (((1,), (0,)), ((), ()))


def split_of(count):
    inner = 1
    for d in range(1, count + 1):
        if count % d == 0 and d * d <= count:
            inner = d
    return inner, count // inner


def named(groups):
    space = types.SimpleNamespace()
    for group in groups:
        for name, value in group.items():
            setattr(space, name, named([value]) if isinstance(value, dict) else value)
    return space


def kernel(seq_count, head_count, tree, *leaves):
    ref = named(jax.tree.unflatten(tree, leaves))
    q_hbm, fresh_hbm, prefill_hbm, res_hbm = ref.q_hbm, ref.fresh_hbm, ref.prefill_hbm, ref.res_hbm
    attn_out, cache_out = ref.attn_out, ref.cache_out
    table, lengths, joins = ref.table, ref.lengths, ref.joins
    arrived = ref.arrived
    inner, outer = split_of(seq_count)
    seq_index = lax.axis_index("seq")
    head_index = lax.axis_index("head")
    group = seq_index // inner

    def fold_back(g, p):
        return jnp.where(lax.rem(g, 2) == 0, p, inner - 1 - p)

    def member(g, p):
        return g * inner + fold_back(g, p)

    place_in = fold_back(group, lax.rem(seq_index, inner))
    step_count, request_count, group_size, head_dim = q_hbm.shape
    rows = step_count * group_size
    resident, res_rows = res_hbm.shape[1], res_hbm.shape[2]
    dev_blocks, block_len = prefill_hbm.shape[2], prefill_hbm.shape[3]
    senders = seq_count * head_count
    slot_count = senders * dev_blocks // seq_count
    per_dev = dev_blocks * block_len
    part, step_part = rows // inner, step_count // inner
    power = math.log2(math.e) / math.sqrt(head_dim)
    heads = [head_index] + [head_index ^ o for o in range(1, head_count)]
    held = ref.held
    staged = ref.staged

    barrier = pltpu.get_barrier_semaphore()

    def greet(**device):
        pl.semaphore_signal(barrier, inc=1, device_id=device, device_id_type=MESH)

    above, below = seq_index + 1 < seq_count, seq_index > 0
    pl.when(above)(lambda: greet(seq=seq_index + 1))
    pl.when(below)(lambda: greet(seq=seq_index - 1))
    for o in range(1, head_count):
        greet(head=heads[o])

    def tell(d):
        if d + 1 < seq_count:
            for sem, there, on, step in ((ref.above_sems, 1, below, -1), (ref.below_sems, -1, above, 1)):
                far = seq_index + there * d

                @pl.when((far >= 0) & (far < seq_count) & on)
                def _(sem=sem, step=step):
                    pl.semaphore_signal(
                        sem.at[d - 1], inc=1, device_id={"seq": seq_index + step}, device_id_type=MESH
                    )

    def learn(d):
        pl.when(seq_index + d < seq_count)(lambda: pl.semaphore_wait(ref.above_sems.at[d - 2], 1))
        pl.when(seq_index - d >= 0)(lambda: pl.semaphore_wait(ref.below_sems.at[d - 2], 1))
        tell(d)

    def local(source, target, sem):
        copy = pltpu.make_async_copy(source, target, sem)
        copy.start()
        return copy

    table_copy = local(ref.table_hbm, table, ref.table_sem)
    own_copy = local(prefill_hbm.at[:, head_index], held[0], ref.own_sem)
    all_copy = local(prefill_hbm, ref.all_buf, ref.all_sem)
    q_copy = local(q_hbm, ref.q_buf, ref.q_sem)
    fresh_copy = local(fresh_hbm, ref.fresh_buf, ref.fresh_sem)
    length_copy = local(ref.lengths_hbm, lengths, ref.lengths_sem)
    join_copy = local(ref.joins_hbm, joins, ref.joins_sem)
    table_copy.wait()
    own_copy.wait()
    chunk = math.gcd(res_rows, 2048)
    chunks = res_rows // chunk
    res_copies = []
    for r in range(resident):
        for k in range(chunks):
            at = pl.ds(k * chunk, chunk)
            res_copies.append(local(res_hbm.at[:, r, at], ref.res_buf.at[:, r, at], ref.res_sems.at[r, k]))

    def remote(source, target, send_sem, recv_sem, **device):
        pltpu.make_async_remote_copy(
            src_ref=source, dst_ref=target, send_sem=send_sem, recv_sem=recv_sem, device_id=device, device_id_type=MESH
        ).start()

    def drain(part_ref, sem):
        pltpu.make_async_copy(part_ref, part_ref, sem).wait()

    def block_for(sender, shard):
        found = jnp.int32(0)
        for k in range(dev_blocks):
            hit = (table[sender * dev_blocks + k] // slot_count) == shard
            found = jnp.where(hit, k, found)
        return found

    def stage(o):
        sender = seq_index * head_count + heads[o]

        def body(z, _):
            found = block_for(sender, z)
            for c in range(2):
                staged[o][z, c] = held[o][c, found]
            return 0

        lax.fori_loop(0, seq_count, body, 0, unroll=seq_count <= 4)
        arrived[seq_index, heads[o]] = staged[o][seq_index]

    def forward(o, distances, inside=None, only=None):
        for d in distances:
            for peer in (seq_index - d, seq_index + d):

                wanted = (peer >= 0) & (peer < seq_count)
                if inside is not None:
                    wanted = wanted & ((peer // inner == group) == inside)

                if only is not None:
                    wanted = wanted & only

                @pl.when(wanted)
                def _(peer=peer):
                    target = arrived.at[seq_index, heads[o]]
                    remote(staged[o].at[peer], target, ref.block_send, ref.block_recv, seq=peer)

    def hand(o):
        remote(ref.all_buf.at[:, heads[o]], held[o], ref.held_send, ref.held_recv.at[o], head=heads[o])

    far_first = range(seq_count - 1, 0, -1)
    stage(0)
    all_copy.wait()
    pl.semaphore_wait(barrier, head_count - 1 + above.astype(jnp.int32) + below.astype(jnp.int32))
    tell(1)
    for o in range(1, head_count):
        hand(o)
    forward(0, [1])
    if seq_count > 2:
        learn(2)
        forward(0, [2])

    def query_rows(r):
        wide = ref.q_buf[:, r].astype(jnp.float32).reshape(rows, head_dim)
        return wide.astype(jnp.bfloat16)

    def fold(carry, q, keys, values, valid):
        s = lax.dot_general(q, keys, NT, preferred_element_type=jnp.float32)
        s = jnp.where(valid, s, very_low)
        top = jnp.max(s, axis=1, keepdims=True)
        if carry is not None:
            top = jnp.maximum(carry[0], top)
        w = jnp.exp2((s - top) * power)
        l = jnp.sum(w, axis=1, keepdims=True)
        acc = lax.dot_general(w.astype(jnp.bfloat16), values, NN, preferred_element_type=jnp.float32)
        if carry is not None:
            keep = jnp.exp2((carry[0] - top) * power)
            l = carry[1] * keep + l
            acc = carry[2] * keep + acc
        return top, l, acc

    length_copy.wait()
    join_copy.wait()
    joined = joins[0, 0]
    q_copy.wait()
    fresh_copy.wait()

    when = lax.broadcasted_iota(jnp.int32, (rows, step_count), 0) // group_size
    which = lax.broadcasted_iota(jnp.int32, (rows, step_count), 1)

    def fold_fresh(carry, r, q):
        allowed = (which <= when) & (seq_index == seq_count - 1)
        if r >= resident:
            allowed = allowed & (which >= joined)
        return fold(carry, q, ref.fresh_buf[0, r], ref.fresh_buf[1, r], allowed)

    def attend_resident(r, between=lambda k: None):
        q = query_rows(r)
        limit = lengths[r] - seq_index * res_rows
        carry = None
        for k in range(chunks):
            res_copies[r * chunks + k].wait()
            at = pl.ds(k * chunk, chunk)
            valid = lax.broadcasted_iota(jnp.int32, (1, chunk), 1) < limit - k * chunk
            carry = fold(carry, q, ref.res_buf[0, r, at], ref.res_buf[1, r, at], valid)
            between(k)
        return fold_fresh(carry, r, q)

    lane = lax.broadcasted_iota(jnp.int32, (rows, rows), 1)

    class Batch:
        def __init__(self, refs, first, results, split):
            self.refs, self.first, self.count, self.split = refs, first, len(results), split and inner > 1
            self.size = part if self.split else rows
            self.mine = pl.ds(pl.multiple_of(place_in * part, part), part) if self.split else slice(0, rows)
            for k, (m, l, acc) in enumerate(results):
                refs.acc[k] = acc
                refs.sent[k] = acc.astype(jnp.bfloat16)
            self.pack(refs.stat, [r[:2] for r in results])
            for oi in range(1, inner):
                to_inner = lax.rem(place_in + oi, inner)
                peer, back = member(group, to_inner), inner - oi
                self.share(refs.stat, back, refs.stat_sems, peer)
                source = refs.sent
                if self.split:
                    source = source.at[:, pl.ds(pl.multiple_of(to_inner * part, part), part)]
                remote(source, refs.got.at[back], refs.got_sems.at[0], refs.got_sems.at[1], seq=peer)

        def pack(self, target, stats):
            count = stats[0][0].shape[0]
            packed = jnp.zeros((count, rows), jnp.float32)
            for k, (m, l) in enumerate(stats):
                packed = jnp.where(lane[0:count] == 2 * k, m, packed)
                packed = jnp.where(lane[0:count] == 2 * k + 1, l, packed)
            if count < rows:
                packed = jnp.concatenate([packed, jnp.zeros((rows - count, rows), jnp.float32)], axis=0)
            tile = jnp.transpose(packed)[0:8]
            target[0:8] = tile
            self.refs.stat_send[0 if target is self.refs.stat else 1] = tile

        def share(self, target, back, sems, peer):
            source = self.refs.stat_send.at[0 if target is self.refs.stat else 1]
            remote(source.at[pl.ds(0, 2 * self.count)], target.at[pl.ds(8 * back, 2 * self.count)], sems.at[0], sems.at[1], seq=peer)

        def columns(self, tiles, members):
            stats = tiles[0 : 8 * members]
            if 8 * members < rows:
                stats = jnp.concatenate([stats, jnp.zeros((rows - 8 * members, rows), jnp.float32)], axis=0)
            return jnp.transpose(stats)

        def combine(self, turned, members, k):
            maxima = [turned[:, 8 * z + 2 * k : 8 * z + 2 * k + 1] for z in members]
            totals = [turned[:, 8 * z + 2 * k + 1 : 8 * z + 2 * k + 2] for z in members]
            top = functools.reduce(jnp.maximum, maxima)
            factors = [jnp.exp2((m - top) * power) for m in maxima]
            return top, sum(f * t for f, t in zip(factors, totals)), factors

        def across(self):
            refs = self.refs
            if inner > 1:
                drain(refs.stat.at[pl.ds(0, 2 * self.count * (inner - 1))], refs.stat_sems.at[1])
            turned = self.columns(refs.stat, inner)
            if self.split:
                ref.turned[...] = turned
                turned = ref.turned[self.mine]
            if inner > 1:
                drain(refs.got.at[pl.ds(1, inner - 1)], refs.got_sems.at[1])
            stats = []
            for k in range(self.count):
                top, total, factors = self.combine(turned, range(inner), k)
                summed = refs.acc[k, self.mine] * factors[0]
                for oi in range(1, inner):
                    summed = summed + refs.got[oi, k].astype(jnp.float32) * factors[oi]
                refs.level[0, k] = (summed / total).astype(jnp.bfloat16)
                stats.append((top, total))
            self.pack(refs.group_stat, stats)
            for og in range(1, outer):
                peer = member(lax.rem(group + og, outer), place_in)
                self.share(refs.group_stat, outer - og, refs.group_sems, peer)
                target = refs.level.at[outer - og]
                remote(refs.level.at[0], target, refs.level_sems.at[0], refs.level_sems.at[1], seq=peer)

        def finish(self):
            refs, level = self.refs, self.refs.level
            drain(refs.group_stat.at[pl.ds(0, 2 * self.count * (outer - 1))], refs.group_sems.at[1])
            turned = self.columns(refs.group_stat, outer)[0 : self.size]
            drain(level.at[pl.ds(1, outer - 1)], refs.level_sems.at[1])
            offset = place_in * step_part if self.split else 0
            steps = pl.ds(offset, self.size // group_size)
            for k in range(self.count):
                _, whole, factors = self.combine(turned, range(outer), k)
                result = jnp.zeros((self.size, head_dim), jnp.float32)
                for g in range(outer):
                    total = turned[:, 8 * g + 2 * k + 1 : 8 * g + 2 * k + 2]
                    result = result + level[g, k].astype(jnp.float32) * (factors[g] * total / whole)
                if self.first + k >= resident:
                    at = lax.broadcasted_iota(jnp.int32, (self.size, head_dim), 0) // group_size
                    result = jnp.where(at + offset >= joined, result, 0.0)
                result = result.reshape(self.size // group_size, group_size, head_dim)
                attn_out[steps, self.first + k] = result.astype(jnp.bfloat16)
            if self.split:
                piece = attn_out.at[steps, pl.ds(self.first, self.count)]
                for oi in range(1, inner):
                    peer = member(group, lax.rem(place_in + oi, inner))
                    remote(piece, piece, refs.final_sems.at[0], refs.final_sems.at[1], seq=peer)

        def close(self):
            refs = self.refs
            if self.split:
                others = attn_out.at[pl.ds(0, step_part * (inner - 1)), pl.ds(self.first, self.count)]
                drain(others, refs.final_sems.at[1])
                drain(others, refs.final_sems.at[0])
            if inner > 1:
                drain(refs.got.at[pl.ds(1, inner - 1)], refs.got_sems.at[0])
                drain(refs.stat.at[pl.ds(0, 2 * self.count * (inner - 1))], refs.stat_sems.at[0])
            drain(refs.group_stat.at[pl.ds(0, 2 * self.count * (outer - 1))], refs.group_sems.at[0])
            drain(refs.level.at[pl.ds(1, outer - 1)], refs.level_sems.at[0])

    def take(o):
        drain(held[o], ref.held_recv.at[o])
        stage(o)

    def between(k):
        if k == 0:
            for d in range(3, seq_count):
                learn(d)
                forward(0, [d])

    results = [attend_resident(0, between)]
    take(1)
    forward(1, far_first, False)
    results += [attend_resident(r) for r in range(1, resident)]
    batch_a = Batch(ref.batch_a, 0, results, True)
    forward(1, far_first, True)
    edge = (seq_index == 0) | (seq_index == seq_count - 1)

    q = query_rows(resident)

    def attend_new(carry, o):
        keys = held[o][0].reshape(per_dev, head_dim)
        values = held[o][1].reshape(per_dev, head_dim)
        base = (seq_index * head_count + heads[o]) * per_dev
        valid = lax.broadcasted_iota(jnp.int32, (1, per_dev), 1) + base < lengths[resident]
        return fold(carry, q, keys, values, valid)

    carry = fold_fresh(None, resident, q)
    for o in range(2):
        carry = attend_new(carry, o)
    for o in range(2, head_count - 1):
        take(o)
        forward(o, far_first, False, edge)
        carry = attend_new(carry, o)
    sources = ref.sources

    def locate(s, _):
        slot = jnp.int32(0)
        for k in range(dev_blocks):
            here = table[s * dev_blocks + k]
            slot = jnp.where((here // slot_count) == seq_index, here, slot)
        ref.slot_of[s] = slot - seq_index * slot_count
        return 0

    lax.fori_loop(0, senders, locate, 0)

    def source_for(j, _):
        def look(s, found):
            return jnp.where(ref.slot_of[s] == j, s, found)

        sources[j] = lax.fori_loop(0, senders, look, jnp.int32(0), unroll=math.gcd(senders, 16))
        return 0

    lax.fori_loop(0, slot_count, source_for, 0)

    batch_a.across()
    last = range(max(head_count - 1, 2), head_count)
    for o in range(2, head_count - 1):
        forward(o, far_first, False, jnp.logical_not(edge))
    for o in last:
        take(o)
        carry = attend_new(carry, o)
    batch_b = Batch(ref.batch_b, resident, [carry], False)
    for o in last:
        forward(o, far_first, False)
    for o in range(2, head_count - 1):
        forward(o, far_first, True)
    batch_b.across()
    for o in last:
        forward(o, far_first, True)
    batch_a.finish()
    batch_b.finish()

    part_ref = arrived.at[pl.ds(0, seq_count - 1)]
    drain(part_ref, ref.block_recv)

    def place(j, _):
        source = sources[j]
        at = pl.ds(pl.multiple_of(j * block_len, block_len), block_len)
        for c in range(2):
            cache_out[c, 0, at] = arrived[source // head_count, lax.rem(source, head_count), c]
        return 0

    lax.fori_loop(0, slot_count, place, 0, unroll=math.gcd(slot_count, 4))
    batch_a.close()
    batch_b.close()
    drain(part_ref, ref.block_send)
    for o in range(1, head_count):
        drain(held[o], ref.held_send)


def store_kernel(attn, cache, attn_out, cache_out, sems):
    copies = [pltpu.make_async_copy(cache.at[c], cache_out.at[c], sems.at[c]) for c in range(2)]
    copies.append(pltpu.make_async_copy(attn, attn_out, sems.at[2]))
    for copy in copies:
        copy.start()
    for copy in copies:
        copy.wait()


def per_device(seq_count, head_count, queries, new_kv, res_kv, prefill_kv, block_table, lengths, join_step):
    step_count, request_count, group_size, head_dim = queries.shape
    rows = step_count * group_size
    resident, res_rows = res_kv.shape[1], res_kv.shape[2]
    head_total, new_rows = prefill_kv.shape[1], prefill_kv.shape[2]
    senders = seq_count * head_count
    dev_blocks = block_table.shape[0] // senders
    block_len = new_rows // dev_blocks
    if dev_blocks != seq_count or resident > 3 or head_total != head_count:
        raise ValueError("unsupported sizes")
    if head_count & (head_count - 1) or head_count < 2 or seq_count < 2 or 8 * seq_count > rows or rows != head_dim:
        raise ValueError("unsupported sizes")
    inner, outer = split_of(seq_count)
    part = rows // inner
    slot_count = block_table.shape[0] // seq_count
    fresh = jnp.transpose(new_kv[:, :, :, 0], (0, 2, 1, 3))
    prefill = prefill_kv.reshape(2, head_total, dev_blocks, block_len, head_dim)
    bf16, f32, i32 = jnp.bfloat16, jnp.float32, jnp.int32
    vmem = pl.BlockSpec(memory_space=pltpu.VMEM)
    hbm = pl.BlockSpec(memory_space=pltpu.HBM)
    chunks = res_rows // math.gcd(res_rows, 2048)
    dma = pltpu.SemaphoreType.DMA
    def vm(dtype, *shape):
        return pltpu.VMEM(shape, dtype)

    def batch(count, size):
        return dict(
            acc=vm(f32, count, rows, head_dim),
            sent=vm(bf16, count, rows, head_dim),
            got=vm(bf16, inner, count, size, head_dim),
            level=vm(bf16, outer, count, size, head_dim),
            stat_send=vm(f32, 2, 8, rows),
            stat=vm(f32, 8 * inner, rows),
            group_stat=vm(f32, 8 * outer, rows),
            stat_sems=dma((2,)),
            group_sems=dma((2,)),
            got_sems=dma((2,)),
            level_sems=dma((2,)),
            final_sems=dma((2,)),
        )

    regular = pltpu.SemaphoreType.REGULAR((max(seq_count - 2, 1),))
    scratch = dict(
        q_buf=vm(bf16, *queries.shape),
        fresh_buf=vm(bf16, *fresh.shape),
        res_buf=vm(bf16, 2, resident, res_rows, head_dim),
        table=pltpu.SMEM(block_table.shape, i32),
        lengths=pltpu.SMEM(lengths.shape, i32),
        joins=pltpu.SMEM((1, 1), i32),
        slot_of=pltpu.SMEM((senders,), i32),
        sources=pltpu.SMEM((slot_count,), i32),
        arrived=vm(bf16, seq_count, head_count, 2, block_len, head_dim),
        turned=vm(f32, rows, rows),
        own_sem=dma,
        all_sem=dma,
        all_buf=vm(bf16, *prefill.shape),
        table_sem=dma,
        q_sem=dma,
        fresh_sem=dma,
        lengths_sem=dma,
        joins_sem=dma,
        res_sems=dma((resident, chunks)),
        block_send=dma,
        block_recv=dma,
        held_send=dma,
        held_recv=dma((head_count,)),
        above_sems=regular,
        below_sems=regular,
        held=[vm(bf16, 2, dev_blocks, block_len, head_dim) for _ in range(head_count)],
        staged=[vm(bf16, seq_count, 2, block_len, head_dim) for _ in range(head_count)],
        batch_a=batch(resident, part),
        batch_b=batch(1, rows),
    )
    inputs = dict(
        q_hbm=queries,
        fresh_hbm=fresh,
        prefill_hbm=prefill,
        table_hbm=block_table,
        lengths_hbm=lengths,
        joins_hbm=join_step.reshape(1, 1),
        res_hbm=res_kv.reshape(2, resident, res_rows, head_dim),
    )
    outputs = dict(
        attn_out=pltpu.VMEM(queries.shape, bf16),
        cache_out=pltpu.VMEM((2, 1, slot_count * block_len, head_dim), bf16),
    )
    operands = jax.tree.leaves(inputs)
    tree = jax.tree.structure((inputs, outputs, scratch))
    out_bytes = 2 * (queries.size + 2 * slot_count * block_len * head_dim)
    attn, cache = pl.pallas_call(
        functools.partial(kernel, seq_count, head_count, tree),
        out_shape=tuple(jax.tree.leaves(outputs)),
        in_specs=[hbm] * len(operands),
        out_specs=(vmem, vmem),
        scratch_shapes=jax.tree.leaves(scratch),
        compiler_params=pltpu.CompilerParams(
            collective_id=0, has_side_effects=True, vmem_limit_bytes=62 * 2**20 - 3 * out_bytes
        ),
    )(*operands)
    return pl.pallas_call(
        store_kernel,
        out_shape=(
            jax.ShapeDtypeStruct(attn.shape, bf16),
            jax.ShapeDtypeStruct(cache.shape, bf16),
        ),
        in_specs=[vmem, vmem],
        out_specs=(hbm, hbm),
        scratch_shapes=[dma((3,))],
        compiler_params=pltpu.CompilerParams(vmem_limit_bytes=2**20),
    )(pltpu.with_memory_space_constraint(attn, pltpu.VMEM), pltpu.with_memory_space_constraint(cache, pltpu.VMEM))


def solution(mesh):
    in_specs = (
        P("groups", None, "head", None),
        P("groups", None, None, "head", None),
        P("groups", None, "seq", "head", None),
        P("groups", None, ("seq", "head"), None),
        P("groups"),
        P("groups"),
        P("groups"),
    )
    out_specs = (P("groups", None, "head", None), P("groups", "head", "seq", None))
    body = functools.partial(per_device, mesh.shape["seq"], mesh.shape["head"])
    return jax.shard_map(body, mesh=mesh, in_specs=in_specs, out_specs=out_specs, check_vma=False)
```
